64 devices in a mesh: dp: 4 (over x, y), sp: 16 (over z, core).
Axes of the slice: x: 2, y: 2, z: 8, core: 2. Of those that a mesh axis runs over, the one named last changes fastest.
The devices are a block of a 4x4x8 slice.
Arguments:
- x_tok: bfloat16 [131072, 1024], P(('dp', 'sp')), parts along dimension 0
- doc_start: int32 [131072], P(('dp', 'sp')), parts along dimension 0
- w_q: bfloat16 [1024, 8, 128], replicated
- w_k: bfloat16 [1024, 8, 128], replicated
- w_v: bfloat16 [1024, 8, 128], replicated
- w_o: bfloat16 [8, 128, 1024], replicated
- dy_tok: bfloat16 [131072, 1024], P(('dp', 'sp')), parts along dimension 0
Outputs:
- output 1: bfloat16 [131072, 1024], P(('dp', 'sp')), parts along dimension 0
- output 2: bfloat16 [131072, 1024], P(('dp', 'sp')), parts along dimension 0
- output 3: float32 [4096, 8, 128], P('dp'), parts along dimension 0
- output 4: float32 [4096, 8, 128], P('dp'), parts along dimension 0
- output 5: float32 [4096, 8, 128], P('dp'), parts along dimension 0
- output 6: float32 [32, 128, 1024], P('dp'), parts along dimension 0
There are 4 independent parts. The reference program is written for one: setup_inputs(seed, part) draws one part's arguments, and reference() takes and returns one part's arrays. A program takes and returns all parts, laid end to end along the dimension named above; an argument that names none is the same for every part.
All inputs are finite; a program needn't handle non-finite values.
Results may differ from the reference program's by a relative error of at most 0.00174767.
Values are sent between devices in bfloat16 or wider.
A program may use at most 768 MiB of HBM per device.

```python
import math
import jax
import jax.numpy as jnp
from jax import lax

D_MODEL = 1024
HEAD_DIM = 128
TOK_DEV = 2048
SEQ_DEVS = 16

NUM_HEADS = D_MODEL // HEAD_DIM
SEQ_LEN = SEQ_DEVS * TOK_DEV
NUM_BOUNDS = SEQ_DEVS // 2 + 1
SCORE_SCALE = 1.0 / (math.sqrt(HEAD_DIM) * TOK_DEV)


def setup_inputs(seed: int = 0, part: int = 0) -> dict:
    key_list = jax.random.split(jax.random.key(seed), 9)
    k_tok = jax.random.fold_in(key_list[0], part)
    k_tok_mean = jax.random.fold_in(key_list[1], part)
    k_grad = jax.random.fold_in(key_list[2], part)
    k_grad_mean = jax.random.fold_in(key_list[3], part)
    k_doc = jax.random.fold_in(key_list[4], part)
    w_scale = D_MODEL ** -0.5
    x_tok = (jax.random.normal(k_tok, (SEQ_LEN, D_MODEL), jnp.float32)
             + jax.random.normal(k_tok_mean, (1, D_MODEL), jnp.float32)).astype(jnp.bfloat16)
    dy_tok = (jax.random.normal(k_grad, (SEQ_LEN, D_MODEL), jnp.float32)
              + jax.random.normal(k_grad_mean, (1, D_MODEL), jnp.float32)).astype(jnp.bfloat16)
    bound_pos = jax.random.randint(k_doc, (NUM_BOUNDS,), 0, SEQ_LEN)
    doc_start = jnp.zeros((SEQ_LEN,), jnp.int32).at[bound_pos].set(1)
    w_q = (jax.random.normal(key_list[5], (D_MODEL, NUM_HEADS, HEAD_DIM), jnp.float32) * w_scale).astype(jnp.bfloat16)
    w_k = (jax.random.normal(key_list[6], (D_MODEL, NUM_HEADS, HEAD_DIM), jnp.float32) * w_scale).astype(jnp.bfloat16)
    w_v = (jax.random.normal(key_list[7], (D_MODEL, NUM_HEADS, HEAD_DIM), jnp.float32) * w_scale).astype(jnp.bfloat16)
    w_o = (jax.random.normal(key_list[8], (NUM_HEADS, HEAD_DIM, D_MODEL), jnp.float32) * w_scale).astype(jnp.bfloat16)
    return {'x_tok': x_tok, 'doc_start': doc_start, 'w_q': w_q, 'w_k': w_k, 'w_v': w_v, 'w_o': w_o, 'dy_tok': dy_tok}


def block_masks(flag_loc):
    positions = jnp.arange(TOK_DEV)
    seg_ids = jnp.cumsum(flag_loc)
    first_pos = jnp.min(jnp.where(flag_loc > 0, positions, TOK_DEV))
    last_pos = jnp.max(jnp.where(flag_loc > 0, positions, -1))
    head_mask = (positions < first_pos).astype(jnp.float32)
    tail_mask = (positions >= last_pos).astype(jnp.float32)
    same_doc = (seg_ids[:, None] == seg_ids[None, :]) & (positions[None, :] <= positions[:, None])
    doc_gate = (last_pos < 0).astype(jnp.float32)
    return head_mask, tail_mask, same_doc, doc_gate


def reference(x_tok, doc_start, w_q, w_k, w_v, w_o, dy_tok):
    wq_mat = w_q.reshape(D_MODEL, D_MODEL)
    wk_mat = w_k.reshape(D_MODEL, D_MODEL)
    wv_mat = w_v.reshape(D_MODEL, D_MODEL)
    wo_mat = w_o.reshape(D_MODEL, D_MODEL)

    def project(x_loc):
        q_rows = jnp.dot(x_loc, wq_mat, preferred_element_type=jnp.float32).astype(jnp.bfloat16).astype(jnp.float32)
        k_rows = jnp.dot(x_loc, wk_mat, preferred_element_type=jnp.float32).astype(jnp.bfloat16).astype(jnp.float32)
        v_rows = jnp.dot(x_loc, wv_mat, preferred_element_type=jnp.float32).astype(jnp.bfloat16).astype(jnp.float32)
        shape3 = (TOK_DEV, NUM_HEADS, HEAD_DIM)
        return q_rows.reshape(shape3), k_rows.reshape(shape3), v_rows.reshape(shape3)

    def forward_step(fwd_state, step_in):
        x_loc, flag_loc = step_in
        head_mask, tail_mask, same_doc, doc_gate = block_masks(flag_loc)
        q_rows, k_rows, v_rows = project(x_loc)
        scores = jnp.einsum('thk,shk->hts', q_rows, k_rows)
        attn_prob = jnp.where(same_doc[None], scores * SCORE_SCALE, 0.0).astype(jnp.bfloat16).astype(jnp.float32)
        intra_sum = jnp.einsum('hts,shv->thv', attn_prob, v_rows)
        state_low = fwd_state.astype(jnp.bfloat16).astype(jnp.float32)
        inter_sum = jnp.einsum('thk,hkv->thv', q_rows, state_low) * (SCORE_SCALE * head_mask)[:, None, None]
        out_rows = (intra_sum + inter_sum).astype(jnp.bfloat16).reshape(TOK_DEV, D_MODEL)
        y_loc = jnp.dot(out_rows, wo_mat, preferred_element_type=jnp.float32).astype(jnp.bfloat16)
        m_tail = jnp.einsum('shk,shv->hkv', k_rows, v_rows * tail_mask[:, None, None])
        next_state = doc_gate * fwd_state + m_tail
        return next_state, (out_rows, y_loc, fwd_state)

    def backward_step(scan_carry, step_in):
        rev_state, acc_q, acc_k, acc_v, acc_o = scan_carry
        x_loc, flag_loc, dy_loc, out_rows, fwd_state = step_in
        head_mask, tail_mask, same_doc, doc_gate = block_masks(flag_loc)
        q_rows, k_rows, v_rows = project(x_loc)
        scores = jnp.einsum('thk,shk->hts', q_rows, k_rows)
        attn_prob = jnp.where(same_doc[None], scores * SCORE_SCALE, 0.0).astype(jnp.bfloat16).astype(jnp.float32)
        d_out = jnp.dot(dy_loc, wo_mat.T, preferred_element_type=jnp.float32).astype(jnp.bfloat16).astype(jnp.float32)
        d_out = d_out.reshape(TOK_DEV, NUM_HEADS, HEAD_DIM)
        dp_raw = jnp.einsum('thv,shv->hts', d_out, v_rows)
        d_prob = jnp.where(same_doc[None], dp_raw * SCORE_SCALE, 0.0).astype(jnp.bfloat16).astype(jnp.float32)
        state_low = fwd_state.astype(jnp.bfloat16).astype(jnp.float32)
        rev_low = rev_state.astype(jnp.bfloat16).astype(jnp.float32)
        head_col = (SCORE_SCALE * head_mask)[:, None, None]
        tail_col = (SCORE_SCALE * tail_mask)[:, None, None]
        dq_rows = (jnp.einsum('hts,shk->thk', d_prob, k_rows)
                   + jnp.einsum('thv,hkv->thk', d_out, state_low) * head_col).astype(jnp.bfloat16).reshape(TOK_DEV, D_MODEL)
        dk_rows = (jnp.einsum('hts,thk->shk', d_prob, q_rows)
                   + jnp.einsum('shv,hkv->shk', v_rows, rev_low) * tail_col).astype(jnp.bfloat16).reshape(TOK_DEV, D_MODEL)
        dv_rows = (jnp.einsum('hts,thv->shv', attn_prob, d_out)
                   + jnp.einsum('shk,hkv->shv', k_rows, rev_low) * tail_col).astype(jnp.bfloat16).reshape(TOK_DEV, D_MODEL)
        dx_loc = (jnp.dot(dq_rows, wq_mat.T, preferred_element_type=jnp.float32)
                  + jnp.dot(dk_rows, wk_mat.T, preferred_element_type=jnp.float32)
                  + jnp.dot(dv_rows, wv_mat.T, preferred_element_type=jnp.float32)).astype(jnp.bfloat16)
        acc_q = acc_q + jnp.dot(x_loc.T, dq_rows, preferred_element_type=jnp.float32)
        acc_k = acc_k + jnp.dot(x_loc.T, dk_rows, preferred_element_type=jnp.float32)
        acc_v = acc_v + jnp.dot(x_loc.T, dv_rows, preferred_element_type=jnp.float32)
        acc_o = acc_o + jnp.dot(out_rows.T, dy_loc, preferred_element_type=jnp.float32)
        n_head = jnp.einsum('thk,thv->hkv', q_rows, d_out * head_mask[:, None, None])
        next_rev = doc_gate * rev_state + n_head
        return (next_rev, acc_q, acc_k, acc_v, acc_o), dx_loc

    x_blocks = x_tok.reshape(SEQ_DEVS, TOK_DEV, D_MODEL)
    flag_blocks = doc_start.reshape(SEQ_DEVS, TOK_DEV)
    dy_blocks = dy_tok.reshape(SEQ_DEVS, TOK_DEV, D_MODEL)
    zero_state = jnp.zeros((NUM_HEADS, HEAD_DIM, HEAD_DIM), jnp.float32)
    last_state, fwd_outs = lax.scan(forward_step, zero_state, (x_blocks, flag_blocks))
    out_blocks, y_blocks, state_blocks = fwd_outs
    zero_grad = jnp.zeros((D_MODEL, D_MODEL), jnp.float32)
    grad_carry, dx_blocks = lax.scan(backward_step, (zero_state, zero_grad, zero_grad, zero_grad, zero_grad),
                                     (x_blocks, flag_blocks, dy_blocks, out_blocks, state_blocks), reverse=True)
    acc_q = grad_carry[1]
    acc_k = grad_carry[2]
    acc_v = grad_carry[3]
    acc_o = grad_carry[4]
    return (y_blocks.reshape(SEQ_LEN, D_MODEL), dx_blocks.reshape(SEQ_LEN, D_MODEL),
            acc_q.reshape(D_MODEL, NUM_HEADS, HEAD_DIM), acc_k.reshape(D_MODEL, NUM_HEADS, HEAD_DIM),
            acc_v.reshape(D_MODEL, NUM_HEADS, HEAD_DIM), acc_o.reshape(NUM_HEADS, HEAD_DIM, D_MODEL))
```

```python
import functools
import math

import jax
import jax.numpy as jnp
from jax import lax
from jax.experimental import pallas as pl
from jax.experimental.pallas import tpu as pltpu
from jax.sharding import PartitionSpec as P

F32 = jnp.float32
BF16 = jnp.bfloat16
MESH = pl.DeviceIdType.MESH
TILE = 256


def dot(lhs, rhs, lhs_dim, rhs_dim):
    return lax.dot_general(lhs, rhs, (((lhs_dim,), (rhs_dim,)), ((), ())), preferred_element_type=F32)


def state_kernel(bounds_ref, q_ref, k_ref, v_ref, do_ref, mn_ref):
    first_pos = bounds_ref[0]
    last_pos = bounds_ref[1]
    rows = lax.broadcasted_iota(jnp.int32, v_ref.shape[1:], 0)
    v_tail = jnp.where(rows >= last_pos, v_ref[0].astype(F32), 0.0).astype(BF16)
    do_head = jnp.where(rows < first_pos, do_ref[0].astype(F32), 0.0).astype(BF16)
    mn_ref[0, 0] = dot(k_ref[0], v_tail, 0, 0)
    mn_ref[1, 0] = dot(q_ref[0], do_head, 0, 0)


def local_states(bounds, q, k, v, do):
    heads, toks, width = q.shape
    row = pl.BlockSpec((1, toks, width), lambda h: (h, 0, 0))
    return pl.pallas_call(
        state_kernel,
        grid=(heads,),
        in_specs=[pl.BlockSpec(memory_space=pltpu.SMEM), row, row, row, row],
        out_specs=pl.BlockSpec((2, 1, width, width), lambda h: (0, h, 0, 0)),
        out_shape=jax.ShapeDtypeStruct((2, heads, width, width), F32),
        cost_estimate=pl.CostEstimate(flops=4 * heads * toks * width * width, bytes_accessed=8 * heads * toks * width,
                                      transcendentals=0),
        name='local_states',
    )(bounds, q, k, v, do)


def chain_kernel(size, heads, mn_ref, gate_ref, out_ref, inbox, outbox, partner, partner_gate, fwd,
                 in_sem, out_sem, fwd_send, fwd_recv, pair_send, pair_recv):
    me = lax.axis_index('sp')
    core = lax.rem(me, 2)
    chip = me // 2
    chips = size // 2
    peer = me + 1 - 2 * core
    step = 4 * core - 2
    nxt = lax.rem(me + step + size, size)
    prv = lax.rem(me - step + size, size)
    is_first = chip == (1 - core) * (chips - 1)
    is_last = chip == core * (chips - 1)
    barrier = pltpu.get_barrier_semaphore()
    for other in (peer, nxt, prv):
        pl.semaphore_signal(barrier, inc=1, device_id={'sp': other}, device_id_type=MESH)
    pl.semaphore_wait(barrier, 3)

    def copy(src, dst, send, recv, dev):
        return pltpu.make_async_remote_copy(src_ref=src, dst_ref=dst, send_sem=send, recv_sem=recv,
                                            device_id={'sp': dev}, device_id_type=MESH)

    give = copy(mn_ref.at[core], partner, pair_send.at[0], pair_recv.at[0], peer)
    give_gate = copy(gate_ref, partner_gate, pair_send.at[1], pair_recv.at[1], peer)
    give.start()
    give_gate.start()

    @pl.when(is_first)
    def _():
        inbox[...] = jnp.zeros_like(inbox)

    give_gate.wait()
    give.wait()
    gate_own = gate_ref[0:1, :]
    gate_peer = partner_gate[0:1, :]

    def hop(h):
        return copy(outbox.at[h], inbox.at[h], out_sem.at[h], in_sem.at[h], nxt)

    def hand(h):
        return copy(inbox.at[h], fwd.at[h], fwd_send.at[h], fwd_recv.at[h], peer)

    def body(h, carry):
        @pl.when(jnp.logical_not(is_first))
        def _():
            hop(h).wait_recv()

        state = gate_peer * inbox[h] + partner[h]

        @pl.when(jnp.logical_not(is_last))
        def _():
            outbox[h] = gate_own * state + mn_ref[1 - core, h]
            hop(h).start()

        hand(h).start()
        out_ref[1 - core, h] = state.astype(BF16)
        return carry

    lax.fori_loop(0, heads, body, 0)

    def finish(h, carry):
        hand(h).wait()
        out_ref[core, h] = fwd[h].astype(BF16)

        @pl.when(jnp.logical_not(is_last))
        def _():
            hop(h).wait_send()

        return carry

    lax.fori_loop(0, heads, finish, 0)


def pass_states(size, mn, gate):
    _, heads, width, _ = mn.shape
    vmem = pl.BlockSpec(memory_space=pltpu.VMEM)
    buf = pltpu.VMEM((heads, width, width), F32)
    return pl.pallas_call(
        functools.partial(chain_kernel, size, heads),
        in_specs=[vmem, vmem],
        out_specs=vmem,
        out_shape=jax.ShapeDtypeStruct(mn.shape, BF16),
        scratch_shapes=[buf, buf, buf, pltpu.VMEM((8, width), F32), buf]
        + [pltpu.SemaphoreType.DMA((heads,))] * 4 + [pltpu.SemaphoreType.DMA((2,))] * 2,
        compiler_params=pltpu.CompilerParams(collective_id=0, has_side_effects=True),
        name='pass_states',
    )(mn, gate)


SLOTS = 4
LAST = 8


def attn_kernel(scale, heads, size, bounds_ref, start_ref, q_ref, k_ref, v_ref, do_ref, st_ref, x_ref, dy_ref,
                o_ref, dq_ref, dk_ref, dv_ref, grad_ref,
                score, part, partner, ring, total, give_send, give_recv, ring_send, ring_recv,
                out_sem, out_send, out_recv):
    toks, width = q_ref.shape[1:]
    tiles = toks // TILE
    first_pos = bounds_ref[0]
    last_pos = bounds_ref[1]
    step = pl.program_id(0)
    me = lax.axis_index('sp')
    core = lax.rem(me, 2)
    chip = me // 2
    chips = size // 2
    peer = me + 1 - 2 * core
    sides = (lax.rem(me + 2, size), lax.rem(me + size - 2, size))
    far = chips // 2

    def copy(src, dst, send, recv, dev):
        return pltpu.make_async_remote_copy(src_ref=src, dst_ref=dst, send_sem=send, recv_sem=recv,
                                            device_id={'sp': dev}, device_id_type=MESH)

    @pl.when(step == 0)
    def _():
        barrier = pltpu.get_barrier_semaphore()
        for other in (peer,) + sides:
            pl.semaphore_signal(barrier, inc=1, device_id={'sp': other}, device_id_type=MESH)
        pl.semaphore_wait(barrier, 3)

    def give(head):
        slot = lax.rem(head, 3)
        return copy(part.at[slot, 1 - core], partner.at[head], give_send.at[slot], give_recv.at[slot], peer)

    def hops(mat, side):
        return far if side == mat else chips - 1 - far

    def sent(mat, side, event):
        count = hops(mat, side)
        return 0 <= event < count or far <= event < far + count

    def chunk(mat, side, event):
        sign = 1 - 2 * side
        if event < far:
            return lax.rem(chip + sign * (hops(mat, side) - event) + chips, chips)
        return lax.rem(chip - sign * (event - far) + chips, chips)

    def ship(head, mat, side, event):
        which = chunk(mat, side, event)
        if event == 0:
            src = partner.at[head, mat, which]
        elif event < far:
            src = ring.at[head, mat, side, event - 1]
        else:
            src = total.at[head, mat, which]
        dst = ring.at[head, mat, side, event] if event < far else total.at[head, mat, which]
        slot = lax.rem(head, 4)
        return copy(src, dst, ring_send.at[slot, mat, side, event], ring_recv.at[slot, mat, side, event], sides[side])

    def outputs(head):
        src = total.at[head]
        dst = grad_ref.at[core, head]
        return (pltpu.make_async_copy(src, dst, out_sem.at[head]),
                copy(src, dst, out_send.at[head], out_recv.at[head], peer))

    def run_event(head, event):
        slot = lax.rem(head, 3)
        if event == 0:
            give(head).wait()
        for mat in range(2):
            for side in ((mat, 1 - mat) if event != far else (1 - mat, mat)):
                if sent(mat, side, event - 1):
                    ship(head, mat, side, event - 1).wait()
                if sent(mat, side, event) and event < far:
                    which = chunk(mat, side, event)
                    if event == 0:
                        partner[head, mat, which] = partner[head, mat, which] + part[slot, core, mat, which]
                    else:
                        ring[head, mat, side, event - 1] = (ring[head, mat, side, event - 1]
                                                            + (part[slot, core, mat, which] + partner[head, mat, which]))
                    ship(head, mat, side, event).start()
                elif sent(mat, side, event) and event > far:
                    ship(head, mat, side, event).start()
            if event == far:
                total[head, mat, chip] = ((ring[head, mat, mat, far - 1] + ring[head, mat, 1 - mat, chips - 2 - far])
                                          + (part[slot, core, mat, chip] + partner[head, mat, chip]))
                ship(head, mat, mat, event).start()
                ship(head, mat, 1 - mat, event).start()
        if event == LAST:
            for out in outputs(head):
                out.start()

    def run_slot(index):
        for back in range(2, -1, -1):
            event = SLOTS * back + index
            if event <= LAST:
                head = step - 1 - back

                @pl.when((head >= 0) & (head < heads))
                def _():
                    run_event(head, event)

    def compute(body):
        pl.when(step < heads)(body)

    def scores(lhs_ref, rhs_ref):
        for i in range(tiles):
            row = pl.ds(i * TILE, TILE)
            left = pl.ds(0, (i + 1) * TILE)
            shape = (TILE, (i + 1) * TILE)
            start = jnp.concatenate([start_ref[row, :]] * (shape[1] // width), axis=1)
            u_pos = lax.broadcasted_iota(jnp.int32, shape, 1)
            seen = (u_pos >= start) & (u_pos <= lax.broadcasted_iota(jnp.int32, shape, 0) + i * TILE)
            score[row, left] = jnp.where(seen, dot(lhs_ref[0, row], rhs_ref[0, left], 1, 1) * scale, 0.0).astype(BF16)

    fwd = st_ref[0, 0]
    rev = st_ref[1, 0]

    def strips(row_ref, row_left, row_add, row_dim, col_ref, col_left, col_add, col_dim):
        for i in range(tiles):
            row = pl.ds(i * TILE, TILE)
            left = pl.ds(0, (i + 1) * TILE)
            below = pl.ds(i * TILE, toks - i * TILE)
            t_pos = lax.broadcasted_iota(jnp.int32, (TILE, width), 0) + i * TILE
            row_ref[0, row] = (dot(score[row, left], row_left[0, left], 1, 0)
                               + jnp.where(t_pos < first_pos, dot(row_add[0, row], fwd, 1, row_dim) * scale, 0.0)
                               ).astype(BF16)
            col_ref[0, row] = (dot(score[below, row], col_left[0, below], 0, 0)
                               + jnp.where(t_pos >= last_pos, dot(col_add[0, row], rev, 1, col_dim) * scale, 0.0)
                               ).astype(BF16)

    @compute
    def _():
        scores(q_ref, k_ref)

    run_slot(0)

    @compute
    def _():
        strips(o_ref, v_ref, q_ref, 0, dv_ref, do_ref, k_ref, 0)

    run_slot(1)

    @compute
    def _():
        scores(do_ref, v_ref)

    run_slot(2)

    @compute
    def _():
        strips(dq_ref, k_ref, do_ref, 1, dk_ref, q_ref, v_ref, 1)

    run_slot(3)

    @compute
    def _():
        slot = lax.rem(step, 3)
        rows = jnp.concatenate([dq_ref[0], dk_ref[0], dv_ref[0]], axis=1)
        cut = 2 * width
        for j in range(x_ref.shape[1] // cut):
            col = pl.ds(j * cut, cut)
            grads = dot(rows, x_ref[:, col], 0, 0)
            grad_o = dot(o_ref[0], dy_ref[:, col], 0, 0)
            for n in range(2):
                for mat in range(3):
                    block = grads[mat * width:(mat + 1) * width, n * width:(n + 1) * width]
                    part[slot, mat // 2, mat % 2, 2 * j + n] = block.T
                part[slot, 1, 1, 2 * j + n] = grad_o[:, n * width:(n + 1) * width]
        give(step).start()

    @pl.when(step == heads + 2)
    def _():
        for head in range(heads):
            for out in outputs(head):
                out.wait()


def attention(scale, size, bounds, start, q, k, v, do, states, x, dy):
    heads, toks, width = q.shape
    model = x.shape[1]
    chips = size // 2
    chunk = model // chips
    once = pl.Buffered(1)
    row = pl.BlockSpec((1, toks, width), lambda h: (jnp.minimum(h, heads - 1), 0, 0))
    whole = pl.BlockSpec((toks, model), lambda h: (0, 0), pipeline_mode=once)
    out = jax.ShapeDtypeStruct(q.shape, BF16)
    block = (chips, chunk, width)
    dma = pltpu.SemaphoreType.DMA
    return pl.pallas_call(
        functools.partial(attn_kernel, scale, heads, size),
        grid=(heads + 3,),
        in_specs=[pl.BlockSpec(memory_space=pltpu.SMEM),
                  pl.BlockSpec((toks, width), lambda h: (0, 0), pipeline_mode=once),
                  row, row, row, row,
                  pl.BlockSpec((2, 1, width, width), lambda h: (0, jnp.minimum(h, heads - 1), 0, 0)),
                  whole, whole],
        out_specs=[row] * 4 + [pl.BlockSpec(memory_space=pl.ANY)],
        out_shape=[out] * 4 + [jax.ShapeDtypeStruct((2, heads, 2) + block, F32)],
        scratch_shapes=[pltpu.VMEM((toks, toks), BF16),
                        pltpu.VMEM((3, 2, 2) + block, F32),
                        pltpu.VMEM((heads, 2) + block, F32),
                        pltpu.VMEM((heads, 2, 2, chips // 2, chunk, width), F32),
                        pltpu.VMEM((heads, 2) + block, F32),
                        dma((3,)), dma((3,)), dma((4, 2, 2, 8)), dma((4, 2, 2, 8)),
                        dma((heads,)), dma((heads,)), dma((heads,))],
        compiler_params=pltpu.CompilerParams(collective_id=1, has_side_effects=True,
                                             vmem_limit_bytes=62 * 2**20,
                                             dimension_semantics=('arbitrary',)),
        cost_estimate=pl.CostEstimate(flops=6 * heads * toks * toks * width, bytes_accessed=16 * heads * toks * width,
                                      transcendentals=0),
        name='attention',
    )(bounds, start, q, k, v, do, states, x, dy)


def solution(mesh):
    seq_devs = mesh.shape['sp']

    def device_body(x_loc, flag_loc, w_q, w_k, w_v, w_o, dy_loc):
        toks = x_loc.shape[0]
        width = w_q.shape[2]
        scale = 1.0 / (math.sqrt(width) * toks)
        pos = jnp.arange(toks, dtype=jnp.int32)
        is_start = flag_loc > 0
        first_pos = jnp.min(jnp.where(is_start, pos, toks))
        last_pos = jnp.max(jnp.where(is_start, pos, -1))
        bounds = jnp.stack([first_pos, last_pos]).astype(jnp.int32)
        start = lax.cummax(jnp.where(is_start, pos, 0))
        start = jnp.broadcast_to(start[:, None], (toks, width))
        gate = jnp.broadcast_to((last_pos < 0).astype(F32), (8, width))

        def project(rows, w, spec):
            return jnp.einsum(spec, rows, w, preferred_element_type=F32).astype(BF16)

        k = project(x_loc, w_k, 'td,dhk->htk')
        v = project(x_loc, w_v, 'td,dhk->htk')
        q = project(x_loc, w_q, 'td,dhk->htk')
        do = project(dy_loc, w_o, 'tc,hkc->htk')
        mn = local_states(bounds, q, k, v, do)
        states = pass_states(seq_devs, mn, gate)
        out, dq, dk, dv, grads = attention(scale, seq_devs, bounds, start, q, k, v, do, states, x_loc, dy_loc)
        dw_q, dw_k, dw_v = [grads[n // 2, :, n % 2].transpose(1, 2, 0, 3).reshape(w_q.shape) for n in range(3)]
        dw_o = grads[1, :, 1].transpose(0, 2, 1, 3).reshape(w_o.shape)
        y_loc = jnp.einsum('htk,hkc->tc', out, w_o, preferred_element_type=F32).astype(BF16)
        dx_loc = (jnp.einsum('htk,dhk->td', dq, w_q, preferred_element_type=F32)
                  + jnp.einsum('htk,dhk->td', dk, w_k, preferred_element_type=F32)
                  + jnp.einsum('htk,dhk->td', dv, w_v, preferred_element_type=F32)).astype(BF16)
        return y_loc, dx_loc, dw_q, dw_k, dw_v, dw_o

    row_spec = P(('dp', 'sp'), None)
    flag_spec = P(('dp', 'sp'))
    w_spec = P(None, None, None)
    dw_spec = P('dp', None, None)
    return jax.shard_map(device_body, mesh=mesh,
                         in_specs=(row_spec, flag_spec, w_spec, w_spec, w_spec, w_spec, row_spec),
                         out_specs=(row_spec, row_spec, dw_spec, dw_spec, dw_spec, dw_spec),
                         check_vma=False)
```

```python
import functools
import math

import jax
import jax.numpy as jnp
from jax import lax
from jax.experimental import pallas as pl
from jax.experimental.pallas import tpu as pltpu
from jax.sharding import PartitionSpec as P

F32 = jnp.float32
BF16 = jnp.bfloat16
MESH = pl.DeviceIdType.MESH
TILE = 256


def dot(lhs, rhs, lhs_dim, rhs_dim):
    return lax.dot_general(lhs, rhs, (((lhs_dim,), (rhs_dim,)), ((), ())), preferred_element_type=F32)


ROWS = 512
GROUP = 2


def front_kernel(size, heads, bounds_ref, gate_ref, x_ref, dy_ref, wq_ref, wk_ref, wv_ref, wo_ref,
                 q_ref, k_ref, v_ref, do_ref, out_ref,
                 mn, inbox, outbox, partner, partner_gate, fwd,
                 in_sem, out_sem, fwd_send, fwd_recv, pair_send, pair_recv, gate_send, gate_recv):
    toks = x_ref.shape[0]
    width = q_ref.shape[2]
    first_pos = bounds_ref[0]
    last_pos = bounds_ref[1]
    step = pl.program_id(0)
    me = lax.axis_index('sp')
    core = lax.rem(me, 2)
    chip = me // 2
    chips = size // 2
    peer = me + 1 - 2 * core
    ahead = 4 * core - 2
    nxt = lax.rem(me + ahead + size, size)
    prv = lax.rem(me - ahead + size, size)
    rank = core * chip + (1 - core) * (chips - 1 - chip)

    def copy(src, dst, send, recv, dev):
        return pltpu.make_async_remote_copy(src_ref=src, dst_ref=dst, send_sem=send, recv_sem=recv,
                                            device_id={'sp': dev}, device_id_type=MESH)

    def give(h):
        return copy(mn.at[core, h], partner.at[h], pair_send.at[h], pair_recv.at[h], peer)

    def hop(h):
        return copy(outbox.at[h], inbox.at[h], out_sem.at[h], in_sem.at[h], nxt)

    def hand(h):
        return copy(inbox.at[h], fwd.at[h], fwd_send.at[h], fwd_recv.at[h], peer)

    give_gate = copy(gate_ref, partner_gate, gate_send.at[0], gate_recv.at[0], peer)

    @pl.when(step == 0)
    def _():
        barrier = pltpu.get_barrier_semaphore()
        for other in (peer, nxt, prv):
            pl.semaphore_signal(barrier, inc=1, device_id={'sp': other}, device_id_type=MESH)
        pl.semaphore_wait(barrier, 3)
        give_gate.start()

        @pl.when(rank == 0)
        def _():
            inbox[...] = jnp.zeros_like(inbox)

        give_gate.wait()

    def relay(h):
        give(h).wait()

        @pl.when(rank > 0)
        def _():
            hop(h).wait_recv()

        state = partner_gate[0:1, :] * inbox[h] + partner[h]

        @pl.when(rank < chips - 1)
        def _():
            outbox[h] = gate_ref[0:1, :] * state + mn[1 - core, h]
            hop(h).start()

        hand(h).start()
        out_ref[1 - core, h] = state.astype(BF16)

    def run_slot(index):
        head = (2 * step + index - 2 - rank) // 2 * GROUP
        due = 2 * step + index - 2 - rank

        @pl.when((due >= 0) & (lax.rem(due + 2 * size, 2) == 0) & (head < heads))
        def _():
            for n in range(GROUP):
                relay(head + n)

    def project(rows_ref, w_ref, w_dim, out):
        for i in range(toks // ROWS):
            row = pl.ds(i * ROWS, ROWS)
            block = dot(rows_ref[row, :], w_ref[...], 1, w_dim).astype(BF16)
            for n in range(GROUP):
                out[n, row] = block[:, n * width:(n + 1) * width]

    pos = lax.broadcasted_iota(jnp.int32, (toks, width), 0)

    @pl.when(step * GROUP < heads)
    def _():
        project(x_ref, wv_ref, 0, v_ref)
        project(x_ref, wk_ref, 0, k_ref)
        for n in range(GROUP):
            v_tail = jnp.where(pos >= last_pos, v_ref[n].astype(F32), 0.0).astype(BF16)
            mn[0, step * GROUP + n] = dot(k_ref[n], v_tail, 0, 0)

    run_slot(0)

    @pl.when(step * GROUP < heads)
    def _():
        project(dy_ref, wo_ref, 1, do_ref)
        project(x_ref, wq_ref, 0, q_ref)
        for n in range(GROUP):
            do_head = jnp.where(pos < first_pos, do_ref[n].astype(F32), 0.0).astype(BF16)
            mn[1, step * GROUP + n] = dot(q_ref[n], do_head, 0, 0)
        for n in range(GROUP):
            give(step * GROUP + n).start()

    run_slot(1)

    @pl.when(step == pl.num_programs(0) - 1)
    def _():
        for h in range(heads):
            hand(h).wait()
            out_ref[core, h] = fwd[h].astype(BF16)

            @pl.when(rank < chips - 1)
            def _():
                hop(h).wait_send()


def front(size, bounds, gate, x, dy, w_q, w_k, w_v, w_o, heads):
    toks, model = x.shape
    width = model // heads
    groups = heads // GROUP
    chips = size // 2
    wide = GROUP * width
    once = pl.Buffered(1)
    last = groups - 1
    vmem = pl.BlockSpec(memory_space=pltpu.VMEM)
    whole = pl.BlockSpec((toks, model), lambda g: (0, 0), pipeline_mode=once)
    cols = pl.BlockSpec((model, wide), lambda g: (0, jnp.minimum(g, last)))
    rows = pl.BlockSpec((wide, model), lambda g: (jnp.minimum(g, last), 0))
    out = pl.BlockSpec((GROUP, toks, width), lambda g: (jnp.minimum(g, last), 0, 0))
    buf = pltpu.VMEM((heads, width, width), F32)
    dma = pltpu.SemaphoreType.DMA
    proj = jax.ShapeDtypeStruct((heads, toks, width), BF16)
    return pl.pallas_call(
        functools.partial(front_kernel, size, heads),
        grid=((2 * groups + chips + 1) // 2,),
        in_specs=[pl.BlockSpec(memory_space=pltpu.SMEM), pl.BlockSpec((8, width), lambda g: (0, 0)),
                  whole, whole, cols, cols, cols, rows],
        out_specs=[out] * 4 + [pl.BlockSpec((2, heads, width, width), lambda g: (0, 0, 0, 0))],
        out_shape=[proj] * 4 + [jax.ShapeDtypeStruct((2, heads, width, width), BF16)],
        scratch_shapes=[pltpu.VMEM((2, heads, width, width), F32), buf, buf, buf, pltpu.VMEM((8, width), F32), buf]
        + [dma((heads,))] * 6 + [dma((1,))] * 2,
        compiler_params=pltpu.CompilerParams(collective_id=0, has_side_effects=True,
                                             vmem_limit_bytes=56 * 2**20,
                                             dimension_semantics=('arbitrary',)),
        cost_estimate=pl.CostEstimate(flops=8 * toks * model * model, bytes_accessed=12 * toks * model,
                                      transcendentals=0),
        name='front',
    )(bounds, gate, x, dy, w_q, w_k, w_v, w_o)


SLOTS = 4
LAST = 8


def attn_kernel(scale, heads, size, bounds_ref, start_ref, q_ref, k_ref, v_ref, do_ref, st_ref, x_ref, dy_ref,
                o_ref, dq_ref, dk_ref, dv_ref, grad_ref,
                score, part, partner, ring, total, give_send, give_recv, ring_send, ring_recv,
                out_sem, out_send, out_recv):
    toks, width = q_ref.shape[1:]
    tiles = toks // TILE
    first_pos = bounds_ref[0]
    last_pos = bounds_ref[1]
    step = pl.program_id(0)
    me = lax.axis_index('sp')
    core = lax.rem(me, 2)
    chip = me // 2
    chips = size // 2
    peer = me + 1 - 2 * core
    sides = (lax.rem(me + 2, size), lax.rem(me + size - 2, size))
    far = chips // 2

    def copy(src, dst, send, recv, dev):
        return pltpu.make_async_remote_copy(src_ref=src, dst_ref=dst, send_sem=send, recv_sem=recv,
                                            device_id={'sp': dev}, device_id_type=MESH)

    @pl.when(step == 0)
    def _():
        barrier = pltpu.get_barrier_semaphore()
        for other in (peer,) + sides:
            pl.semaphore_signal(barrier, inc=1, device_id={'sp': other}, device_id_type=MESH)
        pl.semaphore_wait(barrier, 3)

    def give(head):
        slot = lax.rem(head, 3)
        return copy(part.at[slot, 1 - core], partner.at[head], give_send.at[slot], give_recv.at[slot], peer)

    def hops(mat, side):
        return far if side == mat else chips - 1 - far

    def sent(mat, side, event):
        count = hops(mat, side)
        return 0 <= event < count or far <= event < far + count

    def chunk(mat, side, event):
        sign = 1 - 2 * side
        if event < far:
            return lax.rem(chip + sign * (hops(mat, side) - event) + chips, chips)
        return lax.rem(chip - sign * (event - far) + chips, chips)

    def ship(head, mat, side, event):
        which = chunk(mat, side, event)
        if event == 0:
            src = partner.at[head, mat, which]
        elif event < far:
            src = ring.at[head, mat, side, event - 1]
        else:
            src = total.at[head, mat, which]
        dst = ring.at[head, mat, side, event] if event < far else total.at[head, mat, which]
        slot = lax.rem(head, 4)
        return copy(src, dst, ring_send.at[slot, mat, side, event], ring_recv.at[slot, mat, side, event], sides[side])

    def outputs(head):
        src = total.at[head]
        dst = grad_ref.at[core, head]
        return (pltpu.make_async_copy(src, dst, out_sem.at[head]),
                copy(src, dst, out_send.at[head], out_recv.at[head], peer))

    def run_event(head, event):
        slot = lax.rem(head, 3)
        if event == 0:
            give(head).wait()
        for mat in range(2):
            for side in ((mat, 1 - mat) if event != far else (1 - mat, mat)):
                if sent(mat, side, event - 1):
                    ship(head, mat, side, event - 1).wait()
                if sent(mat, side, event) and event < far:
                    which = chunk(mat, side, event)
                    if event == 0:
                        partner[head, mat, which] = partner[head, mat, which] + part[slot, core, mat, which]
                    else:
                        ring[head, mat, side, event - 1] = (ring[head, mat, side, event - 1]
                                                            + (part[slot, core, mat, which] + partner[head, mat, which]))
                    ship(head, mat, side, event).start()
                elif sent(mat, side, event) and event > far:
                    ship(head, mat, side, event).start()
            if event == far:
                total[head, mat, chip] = ((ring[head, mat, mat, far - 1] + ring[head, mat, 1 - mat, chips - 2 - far])
                                          + (part[slot, core, mat, chip] + partner[head, mat, chip]))
                ship(head, mat, mat, event).start()
                ship(head, mat, 1 - mat, event).start()
        if event == LAST:
            for out in outputs(head):
                out.start()

    def run_slot(index):
        for back in range(2, -1, -1):
            event = SLOTS * back + index
            if event <= LAST:
                head = step - 1 - back

                @pl.when((head >= 0) & (head < heads))
                def _():
                    run_event(head, event)

    def compute(body):
        pl.when(step < heads)(body)

    def scores(lhs_ref, rhs_ref):
        for i in range(tiles):
            row = pl.ds(i * TILE, TILE)
            left = pl.ds(0, (i + 1) * TILE)
            shape = (TILE, (i + 1) * TILE)
            start = jnp.concatenate([start_ref[row, :]] * (shape[1] // width), axis=1)
            u_pos = lax.broadcasted_iota(jnp.int32, shape, 1)
            seen = (u_pos >= start) & (u_pos <= lax.broadcasted_iota(jnp.int32, shape, 0) + i * TILE)
            score[row, left] = jnp.where(seen, dot(lhs_ref[0, row], rhs_ref[0, left], 1, 1) * scale, 0.0).astype(BF16)

    fwd = st_ref[0, 0]
    rev = st_ref[1, 0]

    def strips(row_ref, row_left, row_add, row_dim, col_ref, col_left, col_add, col_dim):
        for i in range(tiles):
            row = pl.ds(i * TILE, TILE)
            left = pl.ds(0, (i + 1) * TILE)
            below = pl.ds(i * TILE, toks - i * TILE)
            t_pos = lax.broadcasted_iota(jnp.int32, (TILE, width), 0) + i * TILE
            row_ref[0, row] = (dot(score[row, left], row_left[0, left], 1, 0)
                               + jnp.where(t_pos < first_pos, dot(row_add[0, row], fwd, 1, row_dim) * scale, 0.0)
                               ).astype(BF16)
            col_ref[0, row] = (dot(score[below, row], col_left[0, below], 0, 0)
                               + jnp.where(t_pos >= last_pos, dot(col_add[0, row], rev, 1, col_dim) * scale, 0.0)
                               ).astype(BF16)

    @compute
    def _():
        scores(q_ref, k_ref)

    run_slot(0)

    @compute
    def _():
        strips(o_ref, v_ref, q_ref, 0, dv_ref, do_ref, k_ref, 0)

    run_slot(1)

    @compute
    def _():
        scores(do_ref, v_ref)

    run_slot(2)

    @compute
    def _():
        strips(dq_ref, k_ref, do_ref, 1, dk_ref, q_ref, v_ref, 1)

    run_slot(3)

    @compute
    def _():
        slot = lax.rem(step, 3)
        rows = jnp.concatenate([dq_ref[0], dk_ref[0], dv_ref[0]], axis=1)
        cut = 2 * width
        for j in range(x_ref.shape[1] // cut):
            col = pl.ds(j * cut, cut)
            grads = dot(rows, x_ref[:, col], 0, 0)
            grad_o = dot(o_ref[0], dy_ref[:, col], 0, 0)
            for n in range(2):
                for mat in range(3):
                    block = grads[mat * width:(mat + 1) * width, n * width:(n + 1) * width]
                    part[slot, mat // 2, mat % 2, 2 * j + n] = block.T
                part[slot, 1, 1, 2 * j + n] = grad_o[:, n * width:(n + 1) * width]
        give(step).start()

    @pl.when(step == heads + 2)
    def _():
        for head in range(heads):
            for out in outputs(head):
                out.wait()


def attention(scale, size, bounds, start, q, k, v, do, states, x, dy):
    heads, toks, width = q.shape
    model = x.shape[1]
    chips = size // 2
    chunk = model // chips
    once = pl.Buffered(1)
    row = pl.BlockSpec((1, toks, width), lambda h: (jnp.minimum(h, heads - 1), 0, 0))
    whole = pl.BlockSpec((toks, model), lambda h: (0, 0), pipeline_mode=once)
    out = jax.ShapeDtypeStruct(q.shape, BF16)
    block = (chips, chunk, width)
    dma = pltpu.SemaphoreType.DMA
    return pl.pallas_call(
        functools.partial(attn_kernel, scale, heads, size),
        grid=(heads + 3,),
        in_specs=[pl.BlockSpec(memory_space=pltpu.SMEM),
                  pl.BlockSpec((toks, width), lambda h: (0, 0), pipeline_mode=once),
                  row, row, row, row,
                  pl.BlockSpec((2, 1, width, width), lambda h: (0, jnp.minimum(h, heads - 1), 0, 0)),
                  whole, whole],
        out_specs=[row] * 4 + [pl.BlockSpec(memory_space=pl.ANY)],
        out_shape=[out] * 4 + [jax.ShapeDtypeStruct((2, heads, 2) + block, F32)],
        scratch_shapes=[pltpu.VMEM((toks, toks), BF16),
                        pltpu.VMEM((3, 2, 2) + block, F32),
                        pltpu.VMEM((heads, 2) + block, F32),
                        pltpu.VMEM((heads, 2, 2, chips // 2, chunk, width), F32),
                        pltpu.VMEM((heads, 2) + block, F32),
                        dma((3,)), dma((3,)), dma((4, 2, 2, 8)), dma((4, 2, 2, 8)),
                        dma((heads,)), dma((heads,)), dma((heads,))],
        compiler_params=pltpu.CompilerParams(collective_id=1, has_side_effects=True,
                                             vmem_limit_bytes=62 * 2**20,
                                             dimension_semantics=('arbitrary',)),
        cost_estimate=pl.CostEstimate(flops=6 * heads * toks * toks * width, bytes_accessed=16 * heads * toks * width,
                                      transcendentals=0),
        name='attention',
    )(bounds, start, q, k, v, do, states, x, dy)


def finish_kernel(o_ref, dq_ref, dk_ref, dv_ref, wq_ref, wk_ref, wv_ref, wo_ref, grad_ref,
                  y_ref, dx_ref, gq_ref, gk_ref, gv_ref, go_ref):
    heads, rows, width = o_ref.shape
    chunks, chunk = grad_ref.shape[3:5]

    def flat(ref):
        return jnp.concatenate([ref[h] for h in range(heads)], axis=1)

    y_ref[...] = dot(flat(o_ref), wo_ref[...], 1, 0).astype(BF16)
    for n, out in enumerate((gq_ref, gk_ref, gv_ref)):
        for j in range(chunks):
            for h in range(heads):
                out[j * chunk:(j + 1) * chunk, h, :] = grad_ref[n // 2, h, n % 2, j]
    for j in range(chunks):
        for h in range(heads):
            go_ref[h, :, j * chunk:(j + 1) * chunk] = grad_ref[1, h, 1, j]
    dx_ref[...] = (dot(flat(dq_ref), wq_ref[...], 1, 1) + dot(flat(dk_ref), wk_ref[...], 1, 1)
                   + dot(flat(dv_ref), wv_ref[...], 1, 1)).astype(BF16)


def finish(out, dq, dk, dv, w_q, w_k, w_v, w_o, grads):
    heads, toks, width = out.shape
    model = w_o.shape[1]
    tiles = toks // ROWS
    chunks, chunk = grads.shape[3:5]
    per = chunks // tiles
    part = pl.BlockSpec((heads, ROWS, width), lambda i: (0, i, 0))
    whole = pl.BlockSpec((model, model), lambda i: (0, 0), pipeline_mode=pl.Buffered(1))
    row = pl.BlockSpec((ROWS, model), lambda i: (i, 0))
    gin = pl.BlockSpec((2, heads, 2, per, chunk, width), lambda i: (0, 0, 0, i, 0, 0))
    gout = pl.BlockSpec((per * chunk, heads, width), lambda i: (i, 0, 0))
    gout_o = pl.BlockSpec((heads, width, per * chunk), lambda i: (0, 0, i))
    act = jax.ShapeDtypeStruct((toks, model), BF16)
    grad = jax.ShapeDtypeStruct((model, heads, width), F32)
    return pl.pallas_call(
        finish_kernel,
        grid=(tiles,),
        in_specs=[part] * 4 + [whole] * 4 + [gin],
        out_specs=[row, row, gout, gout, gout, gout_o],
        out_shape=[act, act, grad, grad, grad, jax.ShapeDtypeStruct((heads, width, model), F32)],
        compiler_params=pltpu.CompilerParams(vmem_limit_bytes=60 * 2**20),
        cost_estimate=pl.CostEstimate(flops=8 * toks * model * model, bytes_accessed=64 * 2**20, transcendentals=0),
        name='finish',
    )(out, dq, dk, dv, w_q, w_k, w_v, w_o, grads)


def solution(mesh):
    seq_devs = mesh.shape['sp']

    def device_body(x_loc, flag_loc, w_q, w_k, w_v, w_o, dy_loc):
        toks = x_loc.shape[0]
        width = w_q.shape[2]
        scale = 1.0 / (math.sqrt(width) * toks)
        pos = jnp.arange(toks, dtype=jnp.int32)
        is_start = flag_loc > 0
        first_pos = jnp.min(jnp.where(is_start, pos, toks))
        last_pos = jnp.max(jnp.where(is_start, pos, -1))
        bounds = jnp.stack([first_pos, last_pos]).astype(jnp.int32)
        start = lax.cummax(jnp.where(is_start, pos, 0))
        start = jnp.broadcast_to(start[:, None], (toks, width))
        gate = jnp.broadcast_to((last_pos < 0).astype(F32), (8, width))

        heads = w_q.shape[1]
        flat_q, flat_k, flat_v = [w.reshape(w.shape[0], heads * width) for w in (w_q, w_k, w_v)]
        flat_o = w_o.reshape(heads * width, w_o.shape[2])
        q, k, v, do, states = front(seq_devs, bounds, gate, x_loc, dy_loc, flat_q, flat_k, flat_v, flat_o, heads)
        out, dq, dk, dv, grads = attention(scale, seq_devs, bounds, start, q, k, v, do, states, x_loc, dy_loc)
        return finish(out, dq, dk, dv, flat_q, flat_k, flat_v, flat_o, grads)

    row_spec = P(('dp', 'sp'), None)
    flag_spec = P(('dp', 'sp'))
    w_spec = P(None, None, None)
    dw_spec = P('dp', None, None)
    return jax.shard_map(device_body, mesh=mesh,
                         in_specs=(row_spec, flag_spec, w_spec, w_spec, w_spec, w_spec, row_spec),
                         out_specs=(row_spec, row_spec, dw_spec, dw_spec, dw_spec, dw_spec),
                         check_vma=False)
```

```python
import functools
import math

import jax
import jax.numpy as jnp
from jax import lax
from jax.experimental import pallas as pl
from jax.experimental.pallas import tpu as pltpu
from jax.sharding import PartitionSpec as P

F32 = jnp.float32
BF16 = jnp.bfloat16
MESH = pl.DeviceIdType.MESH
TILE = 256


def dot(lhs, rhs, lhs_dim, rhs_dim):
    return lax.dot_general(lhs, rhs, (((lhs_dim,), (rhs_dim,)), ((), ())), preferred_element_type=F32)


ROWS = 512
GROUP = 2


def front_kernel(size, heads, bounds_ref, gate_ref, x_ref, dy_ref, wq_ref, wk_ref, wv_ref, wo_ref,
                 q_ref, k_ref, v_ref, do_ref, out_ref,
                 mn, inbox, outbox, partner, partner_gate, fwd,
                 in_sem, out_sem, fwd_send, fwd_recv, pair_send, pair_recv, gate_send, gate_recv):
    toks = x_ref.shape[0]
    width = q_ref.shape[2]
    first_pos = bounds_ref[0]
    last_pos = bounds_ref[1]
    step = pl.program_id(0)
    me = lax.axis_index('sp')
    core = lax.rem(me, 2)
    chip = me // 2
    chips = size // 2
    peer = me + 1 - 2 * core
    ahead = 4 * core - 2
    nxt = lax.rem(me + ahead + size, size)
    prv = lax.rem(me - ahead + size, size)
    rank = core * chip + (1 - core) * (chips - 1 - chip)

    def copy(src, dst, send, recv, dev):
        return pltpu.make_async_remote_copy(src_ref=src, dst_ref=dst, send_sem=send, recv_sem=recv,
                                            device_id={'sp': dev}, device_id_type=MESH)

    def give(h):
        return copy(mn.at[core, h], partner.at[h], pair_send.at[h], pair_recv.at[h], peer)

    def hop(h):
        return copy(outbox.at[h], inbox.at[h], out_sem.at[h], in_sem.at[h], nxt)

    def hand(h):
        return copy(inbox.at[h], fwd.at[h], fwd_send.at[h], fwd_recv.at[h], peer)

    give_gate = copy(gate_ref, partner_gate, gate_send.at[0], gate_recv.at[0], peer)

    @pl.when(step == 0)
    def _():
        barrier = pltpu.get_barrier_semaphore()
        for other in (peer, nxt, prv):
            pl.semaphore_signal(barrier, inc=1, device_id={'sp': other}, device_id_type=MESH)
        pl.semaphore_wait(barrier, 3)
        give_gate.start()

        @pl.when(rank == 0)
        def _():
            inbox[...] = jnp.zeros_like(inbox)

        give_gate.wait()

    def relay(h):
        give(h).wait()

        @pl.when(rank > 0)
        def _():
            hop(h).wait_recv()

        state = partner_gate[0:1, :] * inbox[h] + partner[h]

        @pl.when(rank < chips - 1)
        def _():
            outbox[h] = gate_ref[0:1, :] * state + mn[1 - core, h]
            hop(h).start()

        hand(h).start()
        out_ref[1 - core, h] = state.astype(BF16)

    def run_slot(index):
        head = (2 * step + index - 2 - rank) // 2 * GROUP
        due = 2 * step + index - 2 - rank

        @pl.when((due >= 0) & (lax.rem(due + 2 * size, 2) == 0) & (head < heads))
        def _():
            for n in range(GROUP):
                relay(head + n)

    def project(rows_ref, w_ref, w_dim, out):
        for i in range(toks // ROWS):
            row = pl.ds(i * ROWS, ROWS)
            block = dot(rows_ref[row, :], w_ref[...], 1, w_dim).astype(BF16)
            for n in range(GROUP):
                out[n, row] = block[:, n * width:(n + 1) * width]

    pos = lax.broadcasted_iota(jnp.int32, (toks, width), 0)

    @pl.when(step * GROUP < heads)
    def _():
        project(x_ref, wv_ref, 0, v_ref)
        project(x_ref, wk_ref, 0, k_ref)
        for n in range(GROUP):
            v_tail = jnp.where(pos >= last_pos, v_ref[n].astype(F32), 0.0).astype(BF16)
            mn[0, step * GROUP + n] = dot(k_ref[n], v_tail, 0, 0)

    run_slot(0)

    @pl.when(step * GROUP < heads)
    def _():
        project(dy_ref, wo_ref, 1, do_ref)
        project(x_ref, wq_ref, 0, q_ref)
        for n in range(GROUP):
            do_head = jnp.where(pos < first_pos, do_ref[n].astype(F32), 0.0).astype(BF16)
            mn[1, step * GROUP + n] = dot(q_ref[n], do_head, 0, 0)
        for n in range(GROUP):
            give(step * GROUP + n).start()

    run_slot(1)

    @pl.when(step == pl.num_programs(0) - 1)
    def _():
        for h in range(heads):
            hand(h).wait()
            out_ref[core, h] = fwd[h].astype(BF16)

            @pl.when(rank < chips - 1)
            def _():
                hop(h).wait_send()


def front(size, bounds, gate, x, dy, w_q, w_k, w_v, w_o, heads):
    toks, model = x.shape
    width = model // heads
    groups = heads // GROUP
    chips = size // 2
    wide = GROUP * width
    once = pl.Buffered(1)
    last = groups - 1
    vmem = pl.BlockSpec(memory_space=pltpu.VMEM)
    whole = pl.BlockSpec((toks, model), lambda g: (0, 0), pipeline_mode=once)
    cols = pl.BlockSpec((model, wide), lambda g: (0, jnp.minimum(g, last)))
    rows = pl.BlockSpec((wide, model), lambda g: (jnp.minimum(g, last), 0))
    out = pl.BlockSpec((GROUP, toks, width), lambda g: (jnp.minimum(g, last), 0, 0))
    buf = pltpu.VMEM((heads, width, width), F32)
    dma = pltpu.SemaphoreType.DMA
    proj = jax.ShapeDtypeStruct((heads, toks, width), BF16)
    return pl.pallas_call(
        functools.partial(front_kernel, size, heads),
        grid=((2 * groups + chips + 1) // 2,),
        in_specs=[pl.BlockSpec(memory_space=pltpu.SMEM), pl.BlockSpec((8, width), lambda g: (0, 0)),
                  whole, whole, cols, cols, cols, rows],
        out_specs=[out] * 4 + [pl.BlockSpec((2, heads, width, width), lambda g: (0, 0, 0, 0))],
        out_shape=[proj] * 4 + [jax.ShapeDtypeStruct((2, heads, width, width), BF16)],
        scratch_shapes=[pltpu.VMEM((2, heads, width, width), F32), buf, buf, buf, pltpu.VMEM((8, width), F32), buf]
        + [dma((heads,))] * 6 + [dma((1,))] * 2,
        compiler_params=pltpu.CompilerParams(collective_id=0, has_side_effects=True,
                                             vmem_limit_bytes=56 * 2**20,
                                             dimension_semantics=('arbitrary',)),
        cost_estimate=pl.CostEstimate(flops=8 * toks * model * model, bytes_accessed=12 * toks * model,
                                      transcendentals=0),
        name='front',
    )(bounds, gate, x, dy, w_q, w_k, w_v, w_o)


SLOTS = 3
LAST = 8


def attn_kernel(scale, heads, size, bounds_ref, start_ref, q_ref, k_ref, v_ref, do_ref, st_ref, x_ref, dy_ref,
                o_ref, dq_ref, dk_ref, dv_ref, grad_ref,
                score, part, partner, ring, total, give_send, give_recv, ring_send, ring_recv,
                out_sem, out_send, out_recv):
    toks, width = q_ref.shape[1:]
    tiles = toks // TILE
    first_pos = bounds_ref[0]
    last_pos = bounds_ref[1]
    step = pl.program_id(0)
    me = lax.axis_index('sp')
    core = lax.rem(me, 2)
    chip = me // 2
    chips = size // 2
    peer = me + 1 - 2 * core
    sides = (lax.rem(me + 2, size), lax.rem(me + size - 2, size))
    far = chips // 2

    def copy(src, dst, send, recv, dev):
        return pltpu.make_async_remote_copy(src_ref=src, dst_ref=dst, send_sem=send, recv_sem=recv,
                                            device_id={'sp': dev}, device_id_type=MESH)

    @pl.when(step == 0)
    def _():
        barrier = pltpu.get_barrier_semaphore()
        for other in (peer,) + sides:
            pl.semaphore_signal(barrier, inc=1, device_id={'sp': other}, device_id_type=MESH)
        pl.semaphore_wait(barrier, 3)

    def give(head):
        slot = lax.rem(head, 3)
        return copy(part.at[slot, 1 - core], partner.at[head], give_send.at[slot], give_recv.at[slot], peer)

    def hops(mat, side):
        return far if side == mat else chips - 1 - far

    def sent(mat, side, event):
        count = hops(mat, side)
        return 0 <= event < count or far <= event < far + count

    def chunk(mat, side, event):
        sign = 1 - 2 * side
        if event < far:
            return lax.rem(chip + sign * (hops(mat, side) - event) + chips, chips)
        return lax.rem(chip - sign * (event - far) + chips, chips)

    def ship(head, mat, side, event):
        which = chunk(mat, side, event)
        if event == 0:
            src = partner.at[head, mat, which]
        elif event < far:
            src = ring.at[head, mat, side, event - 1]
        else:
            src = total.at[head, mat, which]
        dst = ring.at[head, mat, side, event] if event < far else total.at[head, mat, which]
        slot = lax.rem(head, 4)
        return copy(src, dst, ring_send.at[slot, mat, side, event], ring_recv.at[slot, mat, side, event], sides[side])

    def outputs(head):
        src = total.at[head]
        dst = grad_ref.at[core, head]
        return (pltpu.make_async_copy(src, dst, out_sem.at[head]),
                copy(src, dst, out_send.at[head], out_recv.at[head], peer))

    def run_event(head, event):
        slot = lax.rem(head, 3)
        if event == 0:
            give(head).wait()
        for mat in range(2):
            for side in ((mat, 1 - mat) if event != far else (1 - mat, mat)):
                if sent(mat, side, event - 1):
                    ship(head, mat, side, event - 1).wait()
                if sent(mat, side, event) and event < far:
                    which = chunk(mat, side, event)
                    if event == 0:
                        partner[head, mat, which] = partner[head, mat, which] + part[slot, core, mat, which]
                    else:
                        ring[head, mat, side, event - 1] = (ring[head, mat, side, event - 1]
                                                            + (part[slot, core, mat, which] + partner[head, mat, which]))
                    ship(head, mat, side, event).start()
                elif sent(mat, side, event) and event > far:
                    ship(head, mat, side, event).start()
            if event == far:
                total[head, mat, chip] = ((ring[head, mat, mat, far - 1] + ring[head, mat, 1 - mat, chips - 2 - far])
                                          + (part[slot, core, mat, chip] + partner[head, mat, chip]))
                ship(head, mat, mat, event).start()
                ship(head, mat, 1 - mat, event).start()
        if event == LAST:
            for out in outputs(head):
                out.start()

    def run_slot(index):
        for back in range(2, -1, -1):
            event = SLOTS * back + index
            if event <= LAST:
                head = step - 1 - back

                @pl.when((head >= 0) & (head < heads))
                def _():
                    run_event(head, event)

    def compute(body):
        pl.when(step < heads)(body)

    def scores(lhs_ref, rhs_ref):
        for i in range(tiles):
            row = pl.ds(i * TILE, TILE)
            left = pl.ds(0, (i + 1) * TILE)
            shape = (TILE, (i + 1) * TILE)
            start = jnp.concatenate([start_ref[row, :]] * (shape[1] // width), axis=1)
            u_pos = lax.broadcasted_iota(jnp.int32, shape, 1)
            seen = (u_pos >= start) & (u_pos <= lax.broadcasted_iota(jnp.int32, shape, 0) + i * TILE)
            score[row, left] = jnp.where(seen, dot(lhs_ref[0, row], rhs_ref[0, left], 1, 1) * scale, 0.0).astype(BF16)

    fwd = st_ref[0, 0]
    rev = st_ref[1, 0]

    def strips(row_ref, row_left, row_add, row_dim, col_ref, col_left, col_add, col_dim):
        for i in range(tiles):
            row = pl.ds(i * TILE, TILE)
            left = pl.ds(0, (i + 1) * TILE)
            below = pl.ds(i * TILE, toks - i * TILE)
            t_pos = lax.broadcasted_iota(jnp.int32, (TILE, width), 0) + i * TILE
            row_ref[0, row] = (dot(score[row, left], row_left[0, left], 1, 0)
                               + jnp.where(t_pos < first_pos, dot(row_add[0, row], fwd, 1, row_dim) * scale, 0.0)
                               ).astype(BF16)
            col_ref[0, row] = (dot(score[below, row], col_left[0, below], 0, 0)
                               + jnp.where(t_pos >= last_pos, dot(col_add[0, row], rev, 1, col_dim) * scale, 0.0)
                               ).astype(BF16)

    def grads(cols):
        slot = lax.rem(step, 3)
        rows = jnp.concatenate([dq_ref[0], dk_ref[0], dv_ref[0]], axis=1)
        cut = 2 * width
        for j in cols:
            col = pl.ds(j * cut, cut)
            grad_rows = dot(rows, x_ref[:, col], 0, 0)
            grad_o = dot(o_ref[0], dy_ref[:, col], 0, 0)
            for n in range(2):
                for mat in range(3):
                    block = grad_rows[mat * width:(mat + 1) * width, n * width:(n + 1) * width]
                    part[slot, mat // 2, mat % 2, 2 * j + n] = block.T
                part[slot, 1, 1, 2 * j + n] = grad_o[:, n * width:(n + 1) * width]

    cuts = x_ref.shape[1] // (2 * width)

    @compute
    def _():
        scores(q_ref, k_ref)

    run_slot(0)

    @compute
    def _():
        strips(o_ref, v_ref, q_ref, 0, dv_ref, do_ref, k_ref, 0)
        scores(do_ref, v_ref)

    run_slot(1)

    @compute
    def _():
        strips(dq_ref, k_ref, do_ref, 1, dk_ref, q_ref, v_ref, 1)
        grads(range(cuts // 2))

    run_slot(2)

    @compute
    def _():
        grads(range(cuts // 2, cuts))
        give(step).start()

    @pl.when(step == heads + 2)
    def _():
        for head in range(heads):
            for out in outputs(head):
                out.wait()


def attention(scale, size, bounds, start, q, k, v, do, states, x, dy):
    heads, toks, width = q.shape
    model = x.shape[1]
    chips = size // 2
    chunk = model // chips
    once = pl.Buffered(1)
    row = pl.BlockSpec((1, toks, width), lambda h: (jnp.minimum(h, heads - 1), 0, 0))
    whole = pl.BlockSpec((toks, model), lambda h: (0, 0), pipeline_mode=once)
    out = jax.ShapeDtypeStruct(q.shape, BF16)
    block = (chips, chunk, width)
    dma = pltpu.SemaphoreType.DMA
    return pl.pallas_call(
        functools.partial(attn_kernel, scale, heads, size),
        grid=(heads + 3,),
        in_specs=[pl.BlockSpec(memory_space=pltpu.SMEM),
                  pl.BlockSpec((toks, width), lambda h: (0, 0), pipeline_mode=once),
                  row, row, row, row,
                  pl.BlockSpec((2, 1, width, width), lambda h: (0, jnp.minimum(h, heads - 1), 0, 0)),
                  whole, whole],
        out_specs=[row] * 4 + [pl.BlockSpec(memory_space=pl.ANY)],
        out_shape=[out] * 4 + [jax.ShapeDtypeStruct((2, heads, 2) + block, F32)],
        scratch_shapes=[pltpu.VMEM((toks, toks), BF16),
                        pltpu.VMEM((3, 2, 2) + block, F32),
                        pltpu.VMEM((heads, 2) + block, F32),
                        pltpu.VMEM((heads, 2, 2, chips // 2, chunk, width), F32),
                        pltpu.VMEM((heads, 2) + block, F32),
                        dma((3,)), dma((3,)), dma((4, 2, 2, 8)), dma((4, 2, 2, 8)),
                        dma((heads,)), dma((heads,)), dma((heads,))],
        compiler_params=pltpu.CompilerParams(collective_id=1, has_side_effects=True,
                                             vmem_limit_bytes=62 * 2**20,
                                             dimension_semantics=('arbitrary',)),
        cost_estimate=pl.CostEstimate(flops=6 * heads * toks * toks * width, bytes_accessed=16 * heads * toks * width,
                                      transcendentals=0),
        name='attention',
    )(bounds, start, q, k, v, do, states, x, dy)


def finish_kernel(o_ref, dq_ref, dk_ref, dv_ref, wq_ref, wk_ref, wv_ref, wo_ref, grad_ref,
                  y_ref, dx_ref, gq_ref, gk_ref, gv_ref, go_ref):
    heads, rows, width = o_ref.shape
    chunks, chunk = grad_ref.shape[3:5]

    def flat(ref):
        return jnp.concatenate([ref[h] for h in range(heads)], axis=1)

    y_ref[...] = dot(flat(o_ref), wo_ref[...], 1, 0).astype(BF16)
    for n, out in enumerate((gq_ref, gk_ref, gv_ref)):
        for j in range(chunks):
            out[j * chunk:(j + 1) * chunk] = jnp.transpose(grad_ref[n // 2, :, n % 2, j], (1, 0, 2))
    for j in range(chunks):
        for h in range(heads):
            go_ref[h, :, j * chunk:(j + 1) * chunk] = grad_ref[1, h, 1, j]
    dx_ref[...] = (dot(flat(dq_ref), wq_ref[...], 1, 1) + dot(flat(dk_ref), wk_ref[...], 1, 1)
                   + dot(flat(dv_ref), wv_ref[...], 1, 1)).astype(BF16)


def finish(out, dq, dk, dv, w_q, w_k, w_v, w_o, grads):
    heads, toks, width = out.shape
    model = w_o.shape[1]
    tiles = toks // TILE
    chunks, chunk = grads.shape[3:5]
    per = chunks // tiles
    part = pl.BlockSpec((heads, TILE, width), lambda i: (0, i, 0))
    whole = pl.BlockSpec((model, model), lambda i: (0, 0), pipeline_mode=pl.Buffered(1))
    row = pl.BlockSpec((TILE, model), lambda i: (i, 0))
    gin = pl.BlockSpec((2, heads, 2, per, chunk, width), lambda i: (0, 0, 0, i, 0, 0))
    gout = pl.BlockSpec((per * chunk, heads, width), lambda i: (i, 0, 0))
    gout_o = pl.BlockSpec((heads, width, per * chunk), lambda i: (0, 0, i))
    act = jax.ShapeDtypeStruct((toks, model), BF16)
    grad = jax.ShapeDtypeStruct((model, heads, width), F32)
    return pl.pallas_call(
        finish_kernel,
        grid=(tiles,),
        in_specs=[part] * 4 + [whole] * 4 + [gin],
        out_specs=[row, row, gout, gout, gout, gout_o],
        out_shape=[act, act, grad, grad, grad, jax.ShapeDtypeStruct((heads, width, model), F32)],
        compiler_params=pltpu.CompilerParams(vmem_limit_bytes=60 * 2**20),
        cost_estimate=pl.CostEstimate(flops=8 * toks * model * model, bytes_accessed=64 * 2**20, transcendentals=0),
        name='finish',
    )(out, dq, dk, dv, w_q, w_k, w_v, w_o, grads)


def solution(mesh):
    seq_devs = mesh.shape['sp']

    def device_body(x_loc, flag_loc, w_q, w_k, w_v, w_o, dy_loc):
        toks = x_loc.shape[0]
        width = w_q.shape[2]
        scale = 1.0 / (math.sqrt(width) * toks)
        pos = jnp.arange(toks, dtype=jnp.int32)
        is_start = flag_loc > 0
        first_pos = jnp.min(jnp.where(is_start, pos, toks))
        last_pos = jnp.max(jnp.where(is_start, pos, -1))
        bounds = jnp.stack([first_pos, last_pos]).astype(jnp.int32)
        start = lax.cummax(jnp.where(is_start, pos, 0))
        start = jnp.broadcast_to(start[:, None], (toks, width))
        gate = jnp.broadcast_to((last_pos < 0).astype(F32), (8, width))

        heads = w_q.shape[1]
        flat_q, flat_k, flat_v = [w.reshape(w.shape[0], heads * width) for w in (w_q, w_k, w_v)]
        flat_o = w_o.reshape(heads * width, w_o.shape[2])
        q, k, v, do, states = front(seq_devs, bounds, gate, x_loc, dy_loc, flat_q, flat_k, flat_v, flat_o, heads)
        out, dq, dk, dv, grads = attention(scale, seq_devs, bounds, start, q, k, v, do, states, x_loc, dy_loc)
        return finish(out, dq, dk, dv, flat_q, flat_k, flat_v, flat_o, grads)

    row_spec = P(('dp', 'sp'), None)
    flag_spec = P(('dp', 'sp'))
    w_spec = P(None, None, None)
    dw_spec = P('dp', None, None)
    return jax.shard_map(device_body, mesh=mesh,
                         in_specs=(row_spec, flag_spec, w_spec, w_spec, w_spec, w_spec, row_spec),
                         out_specs=(row_spec, row_spec, dw_spec, dw_spec, dw_spec, dw_spec),
                         check_vma=False)
```
